512 devices in a mesh: py: 32 (over y, x), pz: 16 (over z, core).
Axes of the slice: x: 4, y: 8, z: 8, core: 2. Of those that a mesh axis runs over, the one named last changes fastest.
Arguments:
- velocity: float32 [3, 320, 320, 320], P(None, 'py', 'pz'), may hold values from -12 to 12
Outputs:
- filtered_velocity: float32 [3, 128, 128, 128], P(None, 'py', 'pz')
- subgrid_stress: float32 [6, 128, 128, 128], P(None, 'py', 'pz')
The draws below stay inside these ranges and needn't reach their ends.
All inputs are finite; a program needn't handle non-finite values.
Results may differ from the reference program's by a relative error of at most 0.000082.
Values sent between devices are 32-bit elements; how exact they have to be, the bound alone decides.
A program may use at most 128 MiB of HBM per device.

```python
import math
import jax
import jax.numpy as jnp

N = 320
M = 128


def block_levels(own_key, shape, pieces, least, largest):
    factor_of = 1.0
    for axis_at, parts in pieces:
        heights = jax.random.uniform(jax.random.fold_in(jax.random.fold_in(own_key, 6), axis_at), (parts,), jnp.float32, least / len(pieces), largest / len(pieces))
        factor_of = factor_of * jnp.repeat(jnp.exp(heights), shape[axis_at] // parts).reshape((-1,) + (1,) * (len(shape) - 1 - axis_at))
    return factor_of


def normal_values(rng, shape, spread, reach, shards=(), kind=jnp.bfloat16):
    drawn = jax.random.normal(rng, shape, jnp.float32) * spread
    if len(shards) > 0:
        drawn = block_levels(rng, shape, shards, -0.22, 0.18) * drawn
    return jnp.clip(drawn, min=-reach, max=reach).astype(kind)


def setup_inputs(seed: int = 0) -> dict:
    keys = jax.random.split(jax.random.key(seed), 2)
    return {
        "velocity": normal_values(keys[0], (3, N, N, N), 2.0, 12.0, ((1, 32), (2, 16)), jnp.float32),
    }


factor_pairs = ((0, 0), (0, 1), (0, 2), (1, 1), (1, 2), (2, 2))


def kept_indices():
    return jnp.concatenate([jnp.arange(M // 2, dtype=jnp.int32), jnp.arange(N - M // 2, N, dtype=jnp.int32)])


def filter_values():
    half_modes = M // 2
    signed_modes = jnp.concatenate([jnp.arange(half_modes, dtype=jnp.int32), jnp.arange(half_modes, dtype=jnp.int32) - half_modes])
    wave_numbers = signed_modes.astype(jnp.float32)
    squares = wave_numbers[:, None, None] ** 2 + wave_numbers[None, :, None] ** 2 + wave_numbers[None, None, :] ** 2
    valid_modes = signed_modes != -half_modes
    retained = valid_modes[:, None, None] & valid_modes[None, :, None] & valid_modes[None, None, :]
    filter_width = 2.0 * math.pi / M
    return jnp.where(retained, jnp.exp(-squares * (filter_width * filter_width / 24.0)), 0.0).astype(jnp.float32)


def filtered_field(fine_field, gain_table, kept_modes):
    spectrum = jnp.take(jnp.fft.fft(fine_field, axis=2), kept_modes, axis=2)
    spectrum = jnp.take(jnp.fft.fft(spectrum, axis=1), kept_modes, axis=1)
    spectrum = jnp.take(jnp.fft.fft(spectrum, axis=0), kept_modes, axis=0)
    coarse = jnp.real(jnp.fft.ifftn(spectrum * gain_table)) * (float(M) ** 3 / float(N) ** 3)
    return jnp.transpose(coarse, (1, 2, 0)).astype(jnp.float32)


def reference(velocity):
    gain_table = filter_values()
    kept_modes = kept_indices()
    coarse = [filtered_field(velocity[component], gain_table, kept_modes) for component in range(3)]
    products = [filtered_field(velocity[left_index] * velocity[right_index], gain_table, kept_modes) for left_index, right_index in factor_pairs]
    filtered = jnp.stack(coarse)
    stress = jnp.stack([products[position] - coarse[left_index] * coarse[right_index] for position, (left_index, right_index) in enumerate(factor_pairs)])
    return filtered, stress
```

```python
import math

import jax
import jax.numpy as jnp
import numpy as np
from jax import lax
from jax.sharding import PartitionSpec as P

N = 320
M = 128

highest = lax.Precision.HIGHEST
factor_pairs = ((0, 0), (0, 1), (0, 2), (1, 1), (1, 2), (2, 2))


def filter_matrix():
    modes = np.arange(-(M // 2) + 1, M // 2)
    gain = np.exp(-(modes**2) * (2.0 * math.pi / M) ** 2 / 24.0)
    points = np.arange(M)[:, None, None] / M - np.arange(N)[None, :, None] / N
    return (np.cos(2.0 * math.pi * modes * points) * gain).sum(-1) / N


def shards(velocity):
    table = jnp.asarray(filter_matrix(), jnp.float32)
    components = [velocity[component] for component in range(3)]
    fields = jnp.stack(components + [components[a] * components[b] for a, b in factor_pairs])
    third = jnp.einsum("fyzx,mx->fyzm", fields, table, precision=highest)
    third = lax.all_to_all(third, "pz", split_axis=3, concat_axis=2, tiled=True)
    second = jnp.einsum("fyzc,mz->fymc", third, table, precision=highest)
    second = lax.all_to_all(second, "py", split_axis=2, concat_axis=1, tiled=True)
    coarse = jnp.einsum("fybc,my->fbcm", second, table, precision=highest)
    stress = jnp.stack(
        [coarse[3 + p] - coarse[a] * coarse[b] for p, (a, b) in enumerate(factor_pairs)]
    )
    return coarse[:3], stress


def solution(mesh):
    placed = P(None, "py", "pz", None)
    return jax.shard_map(
        shards, mesh=mesh, in_specs=(placed,), out_specs=(placed, placed), check_vma=False
    )
```

```python
import math

import jax
import jax.numpy as jnp
import numpy as np
from jax import lax
from jax.experimental import pallas as pl
from jax.experimental.pallas import tpu as pltpu
from jax.sharding import PartitionSpec as P

N = 320
M = 128

factor_pairs = ((0, 0), (0, 1), (0, 2), (1, 1), (1, 2), (2, 2))
FIELDS = 3 + len(factor_pairs)
ROWS = 32
COLS = 16
X1 = N // ROWS
X2 = N // COLS
J = X1 // 2
M2 = M // ROWS
M3 = M // COLS
GROUP = 16
CHUNKS = 3
PIECE = 2 * X2


def filter_matrix():
    modes = np.arange(-(M // 2) + 1, M // 2)
    gain = np.exp(-(modes**2) * (2.0 * math.pi / M) ** 2 / 24.0)
    points = np.arange(M)[:, None, None] / M - np.arange(N)[None, :, None] / N
    return (np.cos(2.0 * math.pi * modes * points) * gain).sum(-1) / N


def tables():
    matrix = filter_matrix()
    blocks = matrix.reshape(ROWS, M2, COLS, X2)
    second = np.zeros((ROWS, 2, M2, COLS, 2, X2))
    for i in range(2):
        second[:, i, :, :, i, :] = blocks
    second = second.reshape(ROWS * 2 * M2, COLS * 2 * X2)
    first = matrix.T.reshape(ROWS, J, 2, M).transpose(1, 0, 2, 3)
    first = np.repeat(first[:, :, :, None, :], M2, axis=3).reshape(J, ROWS * 2 * M2, M)
    return matrix.T.copy(), second, first


def dot(a, b):
    return lax.dot_general(
        a,
        b,
        (((1,), (0,)), ((), ())),
        precision=lax.Precision.HIGHEST,
        preferred_element_type=jnp.float32,
    )


def kernel(
    v_ref,
    third_ref,
    second_hbm,
    first_hbm,
    filtered_ref,
    stress_ref,
    pairs,
    mixed,
    send_z,
    recv_z,
    send_y,
    recv_y,
    second_ref,
    first_ref,
    coarse,
    table_sem,
    send_z_sem,
    recv_z_sem,
    send_y_sem,
    recv_y_sem,
):
    py = lax.axis_index("py")
    pz = lax.axis_index("pz")
    mesh = pl.DeviceIdType.MESH

    barrier = pltpu.get_barrier_semaphore()
    for step in range(1, COLS):
        pl.semaphore_signal(
            barrier, inc=1, device_id={"pz": lax.rem(pz + step, COLS)}, device_id_type=mesh
        )
    for step in range(1, ROWS):
        pl.semaphore_signal(
            barrier, inc=1, device_id={"py": lax.rem(py + step, ROWS)}, device_id_type=mesh
        )

    second_copy = pltpu.make_async_copy(second_hbm, second_ref, table_sem.at[0])
    first_copy = pltpu.make_async_copy(first_hbm, first_ref, table_sem.at[1])
    second_copy.start()
    first_copy.start()

    for c in range(3):
        for j in range(J):
            for i in range(2):
                pairs[c, j, i * X2 : (i + 1) * X2, :] = v_ref[c, 2 * j + i]
    mixed[J * FIELDS :] = jnp.zeros((CHUNKS * GROUP - J * FIELDS, PIECE, M), jnp.float32)
    lanes = lax.broadcasted_iota(jnp.int32, (8, M), 1)

    def third_step(j):
        parts = [pairs[c, j] for c in range(3)]
        parts = parts + [parts[a] * parts[b] for a, b in factor_pairs]
        done = dot(jnp.concatenate(parts, axis=0), third_ref[...])
        mixed[j * FIELDS : (j + 1) * FIELDS] = done.reshape(FIELDS, PIECE, M)

    def spread(c):
        for r in range(PIECE // 8):
            tiles = [mixed[c * GROUP + k, 8 * r : 8 * r + 8, :] for k in range(GROUP)]
            for b in (8, 4, 2, 1):
                low = (lanes // (M3 * b)) % 2 == 0
                for k in range(GROUP):
                    if k & b == 0:
                        x, y = tiles[k], tiles[k + b]
                        tiles[k] = jnp.where(low, x, pltpu.roll(y, M3 * b, 1))
                        tiles[k + b] = jnp.where(low, pltpu.roll(x, M - M3 * b, 1), y)
            for t in range(COLS):
                send_z[c, t, 8 * r : 8 * r + 8, :] = tiles[t]

    def copy_z(c, step):
        target = lax.rem(pz + step, COLS)
        return pltpu.make_async_remote_copy(
            src_ref=send_z.at[c, target],
            dst_ref=recv_z.at[c, pz],
            send_sem=send_z_sem.at[c],
            recv_sem=recv_z_sem.at[c],
            device_id={"pz": target},
            device_id_type=mesh,
        )

    def copy_y(c, step):
        target = lax.rem(py + step, ROWS)
        return pltpu.make_async_remote_copy(
            src_ref=send_y.at[c, target],
            dst_ref=recv_y.at[c, py],
            send_sem=send_y_sem.at[c],
            recv_sem=recv_y_sem.at[c],
            device_id={"py": target},
            device_id_type=mesh,
        )

    def all_z(c):
        return pltpu.make_async_remote_copy(
            src_ref=send_z.at[c, pl.ds(0, COLS - 1)],
            dst_ref=recv_z.at[c, pl.ds(0, COLS - 1)],
            send_sem=send_z_sem.at[c],
            recv_sem=recv_z_sem.at[c],
            device_id={"pz": lax.rem(pz + 1, COLS)},
            device_id_type=mesh,
        )

    def all_y(c):
        return pltpu.make_async_remote_copy(
            src_ref=send_y.at[c, pl.ds(0, ROWS - 1)],
            dst_ref=recv_y.at[c, pl.ds(0, ROWS - 1)],
            send_sem=send_y_sem.at[c],
            recv_sem=recv_y_sem.at[c],
            device_id={"py": lax.rem(py + 1, ROWS)},
            device_id_type=mesh,
        )

    done_j = 0
    for c in range(CHUNKS):
        while done_j < J and done_j * FIELDS < (c + 1) * GROUP:
            third_step(done_j)
            done_j += 1
        spread(c)
        if c == 0:
            pl.semaphore_wait(barrier, COLS + ROWS - 2)
        for step in range(1, COLS):
            copy_z(c, step).start()
        recv_z[c, pz] = send_z[c, pz]

    coarse[...] = jnp.zeros_like(coarse)
    second_copy.wait()
    for c in range(CHUNKS):
        all_z(c).wait_recv()
        done = dot(second_ref[...], recv_z[c].reshape(COLS * PIECE, M))
        send_y[c] = done.reshape(ROWS, 2 * M2, M)
        for step in range(1, ROWS):
            copy_y(c, step).start()
        recv_y[c, py] = send_y[c, py]

    first_copy.wait()
    for c in range(CHUNKS):
        all_y(c).wait_recv()
        turned = recv_y[c].reshape(ROWS * 2 * M2, M).T
        for j in range(J):
            begin = max(j * FIELDS, c * GROUP)
            end = min((j + 1) * FIELDS, (c + 1) * GROUP)
            if begin >= end:
                continue
            rows = turned[M3 * (begin - c * GROUP) : M3 * (end - c * GROUP)]
            mask_of = lax.rem(lax.broadcasted_iota(jnp.int32, rows.shape, 1), M2)
            stacked = jnp.concatenate(
                [jnp.where(mask_of == m, rows, 0.0) for m in range(M2)], axis=0
            )
            done = dot(stacked, first_ref[j])
            fields = end - begin
            coarse[:, begin - j * FIELDS : end - j * FIELDS] += done.reshape(M2, fields, M3, M)

    for m in range(M2):
        parts = [coarse[m, f] for f in range(FIELDS)]
        for f in range(3):
            filtered_ref[f, m] = parts[f]
        for p, (a, b) in enumerate(factor_pairs):
            stress_ref[p, m] = parts[3 + p] - parts[a] * parts[b]

    for c in range(CHUNKS):
        all_z(c).wait_send()
        all_y(c).wait_send()


def shards(velocity):
    third, second, first = (jnp.asarray(table, jnp.float32) for table in tables())
    vmem = pl.BlockSpec(memory_space=pltpu.VMEM)
    anywhere = pl.BlockSpec(memory_space=pl.ANY)
    f32 = jnp.float32
    return pl.pallas_call(
        kernel,
        out_shape=(
            jax.ShapeDtypeStruct((3, M2, M3, M), f32),
            jax.ShapeDtypeStruct((6, M2, M3, M), f32),
        ),
        in_specs=[vmem, vmem, anywhere, anywhere],
        out_specs=(vmem, vmem),
        scratch_shapes=[
            pltpu.VMEM((3, J, PIECE, N), f32),
            pltpu.VMEM((CHUNKS * GROUP, PIECE, M), f32),
            pltpu.VMEM((CHUNKS, COLS, PIECE, M), f32),
            pltpu.VMEM((CHUNKS, COLS, PIECE, M), f32),
            pltpu.VMEM((CHUNKS, ROWS, 2 * M2, M), f32),
            pltpu.VMEM((CHUNKS, ROWS, 2 * M2, M), f32),
            pltpu.VMEM((ROWS * 2 * M2, COLS * PIECE), f32),
            pltpu.VMEM((J, ROWS * 2 * M2, M), f32),
            pltpu.VMEM((M2, FIELDS, M3, M), f32),
            pltpu.SemaphoreType.DMA((2,)),
            pltpu.SemaphoreType.DMA((CHUNKS,)),
            pltpu.SemaphoreType.DMA((CHUNKS,)),
            pltpu.SemaphoreType.DMA((CHUNKS,)),
            pltpu.SemaphoreType.DMA((CHUNKS,)),
        ],
        compiler_params=pltpu.CompilerParams(collective_id=0, has_side_effects=True),
    )(velocity, third, second, first)


def solution(mesh):
    placed = P(None, "py", "pz", None)
    return jax.shard_map(
        shards, mesh=mesh, in_specs=(placed,), out_specs=(placed, placed), check_vma=False
    )
```

```python
import math

import jax
import jax.numpy as jnp
import numpy as np
from jax import lax
from jax.experimental import pallas as pl
from jax.experimental.pallas import tpu as pltpu
from jax.sharding import PartitionSpec as P

N = 320
M = 128

factor_pairs = ((0, 0), (0, 1), (0, 2), (1, 1), (1, 2), (2, 2))
FIELDS = 3 + len(factor_pairs)
ROWS = 32
COLS = 16
X1 = N // ROWS
X2 = N // COLS
X2P = 24
M2 = M // ROWS
M3 = M // COLS
GROUP = 16
CHUNKS = -(-X1 * FIELDS // GROUP)
PLANES = (0, 1, 3, 2, 7, 4, 6, 5)


def filter_matrix():
    modes = np.arange(-(M // 2) + 1, M // 2)
    gain = np.exp(-(modes**2) * (2.0 * math.pi / M) ** 2 / 24.0)
    points = np.arange(M)[:, None, None] / M - np.arange(N)[None, :, None] / N
    return (np.cos(2.0 * math.pi * modes * points) * gain).sum(-1) / N


def tables():
    matrix = filter_matrix()
    second = np.zeros((M, COLS, X2P))
    second[:, :, :X2] = matrix.reshape(M, COLS, X2)
    first = np.repeat(matrix.T.reshape(ROWS, X1, M).transpose(1, 0, 2), M2, axis=1)
    return matrix.T.copy(), second.reshape(M, COLS * X2P), first


def dot(a, b):
    return lax.dot_general(
        a,
        b,
        (((1,), (0,)), ((), ())),
        precision=lax.Precision.HIGH,
        preferred_element_type=jnp.float32,
    )


def kernel(
    v_hbm,
    third_hbm,
    second_hbm,
    first_hbm,
    coarse_ref,
    v_ref,
    third_ref,
    second_ref,
    first_ref,
    mixed,
    send_z,
    recv_z,
    send_y,
    recv_y,
    v_sem,
    table_sem,
    send_z_sem,
    recv_z_sem,
    send_y_sem,
    recv_y_sem,
):
    py = lax.axis_index("py")
    pz = lax.axis_index("pz")
    mesh = pl.DeviceIdType.MESH

    v_copies = [
        pltpu.make_async_copy(v_hbm.at[:, x], v_ref.at[:, x], v_sem.at[x]) for x in range(X1)
    ]
    third_copy = pltpu.make_async_copy(third_hbm, third_ref, table_sem.at[0])
    second_copy = pltpu.make_async_copy(second_hbm, second_ref, table_sem.at[1])
    first_copy = pltpu.make_async_copy(first_hbm, first_ref, table_sem.at[2])
    third_copy.start()
    for copy in v_copies:
        copy.start()
    second_copy.start()
    first_copy.start()

    barrier = pltpu.get_barrier_semaphore()
    for step in range(1, COLS):
        pl.semaphore_signal(
            barrier, inc=1, device_id={"pz": lax.rem(pz + step, COLS)}, device_id_type=mesh
        )
    for step in range(1, ROWS):
        pl.semaphore_signal(
            barrier, inc=1, device_id={"py": lax.rem(py + step, ROWS)}, device_id_type=mesh
        )

    mixed[X1 * FIELDS :] = jnp.zeros((CHUNKS * GROUP - X1 * FIELDS, X2P, M), jnp.float32)
    recv_z[:, :, X2:, :] = jnp.zeros((CHUNKS, COLS, X2P - X2, M), jnp.float32)
    lanes = lax.broadcasted_iota(jnp.int32, (8, M), 1)

    def third_step(x):
        v_copies[x].wait()
        pad = jnp.zeros((X2P - X2, N), jnp.float32)
        parts = [jnp.concatenate([v_ref[c, x], pad], axis=0) for c in range(3)]
        parts = parts + [parts[a] * parts[b] for a, b in factor_pairs]
        done = dot(jnp.concatenate(parts, axis=0), third_ref[...])
        mixed[x * FIELDS : (x + 1) * FIELDS] = done.reshape(FIELDS, X2P, M)

    def spread(c):
        for r in range(X2P // 8):
            tiles = [mixed[c * GROUP + k, 8 * r : 8 * r + 8, :] for k in range(GROUP)]
            for b in (8, 4, 2, 1):
                low = (lanes // (M3 * b)) % 2 == 0
                for k in range(GROUP):
                    if k & b == 0:
                        x, y = tiles[k], tiles[k + b]
                        tiles[k] = jnp.where(low, x, pltpu.roll(y, M3 * b, 1))
                        tiles[k + b] = jnp.where(low, pltpu.roll(x, M - M3 * b, 1), y)
            for t in range(COLS):
                send_z[c, t, 8 * r : 8 * r + 8, :] = tiles[t]

    def copy_z(c, target):
        return pltpu.make_async_remote_copy(
            src_ref=send_z.at[c, target, pl.ds(0, X2)],
            dst_ref=recv_z.at[c, pz, pl.ds(0, X2)],
            send_sem=send_z_sem.at[c],
            recv_sem=recv_z_sem.at[c],
            device_id={"pz": target},
            device_id_type=mesh,
        )

    def send_planes(c):
        for plane in PLANES:
            for core in range(2):
                target = 2 * plane + core

                @pl.when(pz != target)
                def _():
                    copy_z(c, target).start()

    def copy_y(c, step):
        target = lax.rem(py + step, ROWS)
        return pltpu.make_async_remote_copy(
            src_ref=send_y.at[c, pl.ds(M2 * target, M2)],
            dst_ref=recv_y.at[c, pl.ds(M2 * py, M2)],
            send_sem=send_y_sem.at[c],
            recv_sem=recv_y_sem.at[c],
            device_id={"py": target},
            device_id_type=mesh,
        )

    def all_z(c):
        return pltpu.make_async_remote_copy(
            src_ref=send_z.at[c, pl.ds(0, COLS - 1), pl.ds(0, X2)],
            dst_ref=recv_z.at[c, pl.ds(0, COLS - 1), pl.ds(0, X2)],
            send_sem=send_z_sem.at[c],
            recv_sem=recv_z_sem.at[c],
            device_id={"pz": lax.rem(pz + 1, COLS)},
            device_id_type=mesh,
        )

    def all_y(c):
        return pltpu.make_async_remote_copy(
            src_ref=send_y.at[c, pl.ds(0, M2 * (ROWS - 1))],
            dst_ref=recv_y.at[c, pl.ds(0, M2 * (ROWS - 1))],
            send_sem=send_y_sem.at[c],
            recv_sem=recv_y_sem.at[c],
            device_id={"py": lax.rem(py + 1, ROWS)},
            device_id_type=mesh,
        )

    third_copy.wait()
    done_x = 0
    for c in range(CHUNKS):
        while done_x < X1 and done_x * FIELDS < (c + 1) * GROUP:
            third_step(done_x)
            done_x += 1
        spread(c)
        if c == 0:
            pl.semaphore_wait(barrier, COLS + ROWS - 2)
        send_planes(c)
        recv_z[c, pz, :X2] = send_z[c, pz, :X2]

    second_copy.wait()
    for c in range(CHUNKS):
        all_z(c).wait_recv()
        send_y[c] = dot(second_ref[...], recv_z[c].reshape(COLS * X2P, M))
        for step in range(1, ROWS):
            copy_y(c, step).start()

    first_copy.wait()
    coarse = [None] * FIELDS
    place = lax.broadcasted_iota(jnp.int32, (ROWS * M2, M), 0) // M2
    for c in range(CHUNKS):
        all_y(c).wait_recv()
        turned = jnp.where(place == py, send_y[c], recv_y[c]).T
        for x in range(X1):
            begin = max(x * FIELDS, c * GROUP)
            end = min((x + 1) * FIELDS, (c + 1) * GROUP)
            if begin >= end:
                continue
            rows = turned[M3 * (begin - c * GROUP) : M3 * (end - c * GROUP)]
            own = lax.rem(lax.broadcasted_iota(jnp.int32, rows.shape, 1), M2)
            stacked = jnp.concatenate([jnp.where(own == m, rows, 0.0) for m in range(M2)], axis=0)
            done = dot(stacked, first_ref[x]).reshape(M2, end - begin, M3, M)
            for k in range(end - begin):
                f = begin + k - x * FIELDS
                if x == 0:
                    coarse_ref[f] = done[:, k]
                else:
                    coarse_ref[f] += done[:, k]

    for c in range(CHUNKS):
        all_z(c).wait_send()
        all_y(c).wait_send()


def finish(coarse_ref, filtered_ref, stress_ref):
    filtered_ref[...] = coarse_ref[:3]
    for p, (a, b) in enumerate(factor_pairs):
        stress_ref[p] = coarse_ref[3 + p] - coarse_ref[a] * coarse_ref[b]


def shards(velocity):
    third, second, first = (jnp.asarray(table, jnp.float32) for table in tables())
    vmem = pl.BlockSpec(memory_space=pltpu.VMEM)
    anywhere = pl.BlockSpec(memory_space=pl.ANY)
    f32 = jnp.float32
    coarse = pl.pallas_call(
        kernel,
        out_shape=jax.ShapeDtypeStruct((FIELDS, M2, M3, M), f32),
        in_specs=[anywhere] * 4,
        out_specs=vmem,
        scratch_shapes=[
            pltpu.VMEM((3, X1, X2, N), f32),
            pltpu.VMEM((N, M), f32),
            pltpu.VMEM((M, COLS * X2P), f32),
            pltpu.VMEM((X1, ROWS * M2, M), f32),
            pltpu.VMEM((CHUNKS * GROUP, X2P, M), f32),
            pltpu.VMEM((CHUNKS, COLS, X2P, M), f32),
            pltpu.VMEM((CHUNKS, COLS, X2P, M), f32),
            pltpu.VMEM((CHUNKS, ROWS * M2, M), f32),
            pltpu.VMEM((CHUNKS, ROWS * M2, M), f32),
            pltpu.SemaphoreType.DMA((X1,)),
            pltpu.SemaphoreType.DMA((3,)),
            pltpu.SemaphoreType.DMA((CHUNKS,)),
            pltpu.SemaphoreType.DMA((CHUNKS,)),
            pltpu.SemaphoreType.DMA((CHUNKS,)),
            pltpu.SemaphoreType.DMA((CHUNKS,)),
        ],
        compiler_params=pltpu.CompilerParams(collective_id=0, has_side_effects=True),
    )(velocity, third, second, first)
    return pl.pallas_call(
        finish,
        out_shape=(
            jax.ShapeDtypeStruct((3, M2, M3, M), f32),
            jax.ShapeDtypeStruct((6, M2, M3, M), f32),
        ),
        in_specs=[vmem],
        out_specs=(vmem, vmem),
    )(coarse)


def solution(mesh):
    placed = P(None, "py", "pz", None)
    return jax.shard_map(
        shards, mesh=mesh, in_specs=(placed,), out_specs=(placed, placed), check_vma=False
    )
```

```python
import math

import jax
import jax.numpy as jnp
import numpy as np
from jax import lax
from jax.experimental import pallas as pl
from jax.experimental.pallas import tpu as pltpu
from jax.sharding import PartitionSpec as P

N = 320
M = 128

factor_pairs = ((0, 0), (0, 1), (0, 2), (1, 1), (1, 2), (2, 2))
FIELDS = 3 + len(factor_pairs)
ROWS = 32
COLS = 16
X1 = N // ROWS
X2 = N // COLS
X2P = 24
M2 = M // ROWS
M3 = M // COLS
GROUP = 16
CHUNKS = -(-X1 * FIELDS // GROUP)
PLANES = (0, 1, 2, 3, 7, 4, 6, 5)


STEPS = sorted(
    ((down, right) for down in range(8) for right in range(4) if (down, right) != (0, 0)),
    key=lambda step: -min(step[0], 8 - step[0]) - min(step[1], 4 - step[1]),
)


def filter_matrix():
    modes = np.arange(-(M // 2) + 1, M // 2)
    gain = np.exp(-(modes**2) * (2.0 * math.pi / M) ** 2 / 24.0)
    points = np.arange(M)[:, None, None] / M - np.arange(N)[None, :, None] / N
    return (np.cos(2.0 * math.pi * modes * points) * gain).sum(-1) / N


def tables():
    matrix = filter_matrix()
    second = np.zeros((M, COLS, X2P))
    second[:, :, :X2] = matrix.reshape(M, COLS, X2)
    first = np.repeat(matrix.T.reshape(ROWS, X1, M).transpose(1, 0, 2), M2, axis=1)
    return matrix.T.copy(), second.reshape(M, COLS * X2P), first


def dot(a, b):
    return lax.dot_general(
        a,
        b,
        (((1,), (0,)), ((), ())),
        precision=lax.Precision.HIGHEST,
        preferred_element_type=jnp.float32,
    )


def kernel(
    v_hbm,
    third_hbm,
    second_hbm,
    first_hbm,
    coarse_ref,
    v_ref,
    third_ref,
    second_ref,
    first_ref,
    mixed,
    send_z,
    recv_z,
    send_y,
    recv_y,
    v_sem,
    table_sem,
    send_z_sem,
    recv_z_sem,
    send_y_sem,
    recv_y_sem,
):
    py = lax.axis_index("py")
    pz = lax.axis_index("pz")
    mesh = pl.DeviceIdType.MESH

    v_copies = [
        pltpu.make_async_copy(v_hbm.at[:, x], v_ref.at[:, x], v_sem.at[x]) for x in range(X1)
    ]
    third_copy = pltpu.make_async_copy(third_hbm, third_ref, table_sem.at[0])
    second_copy = pltpu.make_async_copy(second_hbm, second_ref, table_sem.at[1])
    first_copy = pltpu.make_async_copy(first_hbm, first_ref, table_sem.at[2])
    third_copy.start()
    for copy in v_copies:
        copy.start()
    second_copy.start()
    first_copy.start()

    barrier = pltpu.get_barrier_semaphore()
    for step in range(1, COLS):
        pl.semaphore_signal(
            barrier, inc=1, device_id={"pz": lax.rem(pz + step, COLS)}, device_id_type=mesh
        )
    for step in range(1, ROWS):
        pl.semaphore_signal(
            barrier, inc=1, device_id={"py": lax.rem(py + step, ROWS)}, device_id_type=mesh
        )

    mixed[X1 * FIELDS :] = jnp.zeros((CHUNKS * GROUP - X1 * FIELDS, X2P, M), jnp.float32)
    recv_z[:, :, X2:, :] = jnp.zeros((CHUNKS, COLS, X2P - X2, M), jnp.float32)
    lanes = lax.broadcasted_iota(jnp.int32, (8, M), 1)

    def third_step(x):
        v_copies[x].wait()
        pad = jnp.zeros((X2P - X2, N), jnp.float32)
        parts = [jnp.concatenate([v_ref[c, x], pad], axis=0) for c in range(3)]
        parts = parts + [parts[a] * parts[b] for a, b in factor_pairs]
        done = dot(jnp.concatenate(parts, axis=0), third_ref[...])
        mixed[x * FIELDS : (x + 1) * FIELDS] = done.reshape(FIELDS, X2P, M)

    def spread(c):
        for r in range(X2P // 8):
            tiles = [mixed[c * GROUP + k, 8 * r : 8 * r + 8, :] for k in range(GROUP)]
            for b in (8, 4, 2, 1):
                low = (lanes // (M3 * b)) % 2 == 0
                for k in range(GROUP):
                    if k & b == 0:
                        x, y = tiles[k], tiles[k + b]
                        tiles[k] = jnp.where(low, x, pltpu.roll(y, M3 * b, 1))
                        tiles[k + b] = jnp.where(low, pltpu.roll(x, M - M3 * b, 1), y)
            for t in range(COLS):
                send_z[c, t, 8 * r : 8 * r + 8, :] = tiles[t]

    def copy_z(c, target):
        return pltpu.make_async_remote_copy(
            src_ref=send_z.at[c, target, pl.ds(0, X2)],
            dst_ref=recv_z.at[c, pz, pl.ds(0, X2)],
            send_sem=send_z_sem.at[c],
            recv_sem=recv_z_sem.at[c],
            device_id={"pz": target},
            device_id_type=mesh,
        )

    def send_planes(c, planes):
        for plane in planes:
            for core in (1, 0):
                target = 2 * plane + core

                @pl.when(pz != target)
                def _():
                    copy_z(c, target).start()

    def copy_y(c, step):
        down, right = step
        target = 4 * lax.rem(py // 4 + down, 8) + lax.rem(lax.rem(py, 4) + right, 4)
        return pltpu.make_async_remote_copy(
            src_ref=send_y.at[c, pl.ds(M2 * target, M2)],
            dst_ref=recv_y.at[c, pl.ds(M2 * py, M2)],
            send_sem=send_y_sem.at[c],
            recv_sem=recv_y_sem.at[c],
            device_id={"py": target},
            device_id_type=mesh,
        )

    def all_z(c):
        return pltpu.make_async_remote_copy(
            src_ref=send_z.at[c, pl.ds(0, COLS - 1), pl.ds(0, X2)],
            dst_ref=recv_z.at[c, pl.ds(0, COLS - 1), pl.ds(0, X2)],
            send_sem=send_z_sem.at[c],
            recv_sem=recv_z_sem.at[c],
            device_id={"pz": lax.rem(pz + 1, COLS)},
            device_id_type=mesh,
        )

    def all_y(c):
        return pltpu.make_async_remote_copy(
            src_ref=send_y.at[c, pl.ds(0, M2 * (ROWS - 1))],
            dst_ref=recv_y.at[c, pl.ds(0, M2 * (ROWS - 1))],
            send_sem=send_y_sem.at[c],
            recv_sem=recv_y_sem.at[c],
            device_id={"py": lax.rem(py + 1, ROWS)},
            device_id_type=mesh,
        )

    third_copy.wait()
    done_x = 0
    for c in range(CHUNKS):
        while done_x < X1 and done_x * FIELDS < (c + 1) * GROUP:
            third_step(done_x)
            done_x += 1
        spread(c)
        if c == 0:
            pl.semaphore_wait(barrier, COLS + ROWS - 2)
        if c < CHUNKS - 2:
            send_planes(c, PLANES)
        recv_z[c, pz, :X2] = send_z[c, pz, :X2]

    for planes in ((0,), (1,), (2,), (3,), (7, 4, 6, 5)):
        for c in range(CHUNKS - 2, CHUNKS):
            send_planes(c, planes)

    second_copy.wait()
    for c in range(CHUNKS):
        all_z(c).wait_recv()
        send_y[c] = dot(second_ref[...], recv_z[c].reshape(COLS * X2P, M))
        for step in STEPS:
            copy_y(c, step).start()

    first_copy.wait()
    coarse = [None] * FIELDS
    place = lax.broadcasted_iota(jnp.int32, (ROWS * M2, M), 0) // M2
    for c in range(CHUNKS):
        all_y(c).wait_recv()
        turned = jnp.where(place == py, send_y[c], recv_y[c]).T
        for x in range(X1):
            begin = max(x * FIELDS, c * GROUP)
            end = min((x + 1) * FIELDS, (c + 1) * GROUP)
            if begin >= end:
                continue
            rows = turned[M3 * (begin - c * GROUP) : M3 * (end - c * GROUP)]
            own = lax.rem(lax.broadcasted_iota(jnp.int32, rows.shape, 1), M2)
            stacked = jnp.concatenate([jnp.where(own == m, rows, 0.0) for m in range(M2)], axis=0)
            done = dot(stacked, first_ref[x]).reshape(M2, end - begin, M3, M)
            for k in range(end - begin):
                f = begin + k - x * FIELDS
                if x == 0:
                    coarse_ref[f] = done[:, k]
                else:
                    coarse_ref[f] += done[:, k]

    for c in range(CHUNKS):
        all_z(c).wait_send()
        all_y(c).wait_send()


def finish(coarse_ref, filtered_ref, stress_ref):
    filtered_ref[...] = coarse_ref[:3]
    for p, (a, b) in enumerate(factor_pairs):
        stress_ref[p] = coarse_ref[3 + p] - coarse_ref[a] * coarse_ref[b]


def shards(velocity):
    third, second, first = (jnp.asarray(table, jnp.float32) for table in tables())
    vmem = pl.BlockSpec(memory_space=pltpu.VMEM)
    anywhere = pl.BlockSpec(memory_space=pl.ANY)
    f32 = jnp.float32
    coarse = pl.pallas_call(
        kernel,
        out_shape=jax.ShapeDtypeStruct((FIELDS, M2, M3, M), f32),
        in_specs=[anywhere] * 4,
        out_specs=vmem,
        scratch_shapes=[
            pltpu.VMEM((3, X1, X2, N), f32),
            pltpu.VMEM((N, M), f32),
            pltpu.VMEM((M, COLS * X2P), f32),
            pltpu.VMEM((X1, ROWS * M2, M), f32),
            pltpu.VMEM((CHUNKS * GROUP, X2P, M), f32),
            pltpu.VMEM((CHUNKS, COLS, X2P, M), f32),
            pltpu.VMEM((CHUNKS, COLS, X2P, M), f32),
            pltpu.VMEM((CHUNKS, ROWS * M2, M), f32),
            pltpu.VMEM((CHUNKS, ROWS * M2, M), f32),
            pltpu.SemaphoreType.DMA((X1,)),
            pltpu.SemaphoreType.DMA((3,)),
            pltpu.SemaphoreType.DMA((CHUNKS,)),
            pltpu.SemaphoreType.DMA((CHUNKS,)),
            pltpu.SemaphoreType.DMA((CHUNKS,)),
            pltpu.SemaphoreType.DMA((CHUNKS,)),
        ],
        compiler_params=pltpu.CompilerParams(collective_id=0, has_side_effects=True, vmem_limit_bytes=24 << 20),
    )(*(pltpu.with_memory_space_constraint(x, pltpu.HBM) for x in (velocity, third, second, first)))
    return pl.pallas_call(
        finish,
        out_shape=(
            jax.ShapeDtypeStruct((3, M2, M3, M), f32),
            jax.ShapeDtypeStruct((6, M2, M3, M), f32),
        ),
        in_specs=[vmem],
        out_specs=(vmem, vmem),
        compiler_params=pltpu.CompilerParams(vmem_limit_bytes=4 << 20),
    )(coarse)


def solution(mesh):
    placed = P(None, "py", "pz", None)
    return jax.shard_map(
        shards, mesh=mesh, in_specs=(placed,), out_specs=(placed, placed), check_vma=False
    )
```

```python
import math

import jax
import jax.numpy as jnp
import numpy as np
from jax import lax
from jax.experimental import pallas as pl
from jax.experimental.pallas import tpu as pltpu
from jax.sharding import PartitionSpec as P

N = 320
M = 128

factor_pairs = ((0, 0), (0, 1), (0, 2), (1, 1), (1, 2), (2, 2))
FIELDS = 3 + len(factor_pairs)
ROWS = 32
COLS = 16
X1 = N // ROWS
X2 = N // COLS
X2P = 24
M2 = M // ROWS
M3 = M // COLS
GROUP = 16
CHUNKS = -(-X1 * FIELDS // GROUP)
STARTS = [max(0, X1 * FIELDS - GROUP * (CHUNKS - c)) for c in range(CHUNKS + 1)]
HALF = M3 * STARTS[1] // 2
FOLD = 7
FOLDS = M // HALF
PLANES = (0, 1, 2, 3, 7, 4, 6, 5)


TARGETS = sorted(
    range(ROWS), key=lambda p: min(p // 4, 8 - p // 4) + min(p % 4, 4 - p % 4)
)


def filter_matrix():
    modes = np.arange(-(M // 2) + 1, M // 2)
    gain = np.exp(-(modes**2) * (2.0 * math.pi / M) ** 2 / 24.0)
    points = np.arange(M)[:, None, None] / M - np.arange(N)[None, :, None] / N
    return (np.cos(2.0 * math.pi * modes * points) * gain).sum(-1) / N


def tables():
    matrix = filter_matrix()
    second = np.zeros((M, COLS, X2P))
    second[:, :, :X2] = matrix.reshape(M, COLS, X2)
    first = np.repeat(matrix.T.reshape(ROWS, X1, M).transpose(1, 0, 2), M2, axis=1)
    return matrix.T.copy(), second.reshape(M, COLS * X2P), first


def dot(a, b):
    return lax.dot_general(
        a,
        b,
        (((1,), (0,)), ((), ())),
        precision=lax.Precision.HIGHEST,
        preferred_element_type=jnp.float32,
    )


def kernel(
    v_hbm,
    third_hbm,
    second_hbm,
    first_hbm,
    coarse_ref,
    v_ref,
    third_ref,
    second_ref,
    first_ref,
    mixed,
    send_z,
    recv_z,
    fold_send,
    fold_recv,
    send_y,
    recv_y,
    v_sem,
    table_sem,
    send_z_sem,
    recv_z_sem,
    send_y_sem,
    recv_y_sem,
):
    py = lax.axis_index("py")
    pz = lax.axis_index("pz")
    mesh = pl.DeviceIdType.MESH

    v_copies = [
        pltpu.make_async_copy(v_hbm.at[:, x], v_ref.at[:, x], v_sem.at[x]) for x in range(X1)
    ]
    third_copy = pltpu.make_async_copy(third_hbm, third_ref, table_sem.at[0])
    second_copy = pltpu.make_async_copy(second_hbm, second_ref, table_sem.at[1])
    first_copy = pltpu.make_async_copy(first_hbm, first_ref, table_sem.at[2])
    third_copy.start()
    for copy in v_copies:
        copy.start()
    second_copy.start()
    first_copy.start()

    barrier = pltpu.get_barrier_semaphore()
    for step in range(1, COLS):
        pl.semaphore_signal(
            barrier, inc=1, device_id={"pz": lax.rem(pz + step, COLS)}, device_id_type=mesh
        )
    for step in range(1, ROWS):
        pl.semaphore_signal(
            barrier, inc=1, device_id={"py": lax.rem(py + step, ROWS)}, device_id_type=mesh
        )

    recv_z[:, :, X2:, :] = jnp.zeros((CHUNKS, COLS, X2P - X2, M), jnp.float32)
    lanes = lax.broadcasted_iota(jnp.int32, (8, M), 1)

    def third_step(x):
        v_copies[x].wait()
        pad = jnp.zeros((X2P - X2, N), jnp.float32)
        parts = [jnp.concatenate([v_ref[c, x], pad], axis=0) for c in range(3)]
        parts = parts + [parts[a] * parts[b] for a, b in factor_pairs]
        done = dot(jnp.concatenate(parts, axis=0), third_ref[...])
        mixed[x * FIELDS : (x + 1) * FIELDS] = done.reshape(FIELDS, X2P, M)

    def spread(c):
        for r in range(X2P // 8):
            pairs = range(STARTS[c], STARTS[c + 1])
            tiles = [mixed[k, 8 * r : 8 * r + 8, :] for k in pairs]
            tiles = tiles + [jnp.zeros((8, M), jnp.float32)] * (GROUP - len(pairs))
            for b in (8, 4, 2, 1):
                low = (lanes // (M3 * b)) % 2 == 0
                for k in range(GROUP):
                    if k & b == 0:
                        x, y = tiles[k], tiles[k + b]
                        tiles[k] = jnp.where(low, x, pltpu.roll(y, M3 * b, 1))
                        tiles[k + b] = jnp.where(low, pltpu.roll(x, M - M3 * b, 1), y)
            for t in range(COLS):
                send_z[c, t, 8 * r : 8 * r + 8, :] = tiles[t]

    def fold():
        for t in range(COLS):
            for half in range(2):
                row = jnp.zeros((8, M), jnp.float32)
                for g in range(FOLDS):
                    part = send_z[0, t, FOLD * g : FOLD * g + 8, :]
                    part = pltpu.roll(part, (HALF * (g - half)) % M, 1) if g != half else part
                    row = jnp.where(lanes // HALF == g, part, row)
                fold_send[t, FOLD * half : FOLD * half + 8, :] = row

    def unfold():
        for t in range(COLS):
            for g in range(FOLDS):
                row = jnp.zeros((8, M), jnp.float32)
                for half in range(2):
                    part = fold_recv[t, FOLD * half : FOLD * half + 8, :]
                    part = pltpu.roll(part, (HALF * (half - g)) % M, 1) if g != half else part
                    row = jnp.where(lanes // HALF == half, part, row)
                kept = min(8, X2 - FOLD * g)
                recv_z[0, t, FOLD * g : FOLD * g + kept, :] = row[:kept]
        recv_z[0, pz, :X2] = send_z[0, pz, :X2]

    def copy_z(c, target):
        if c == 0:
            return pltpu.make_async_remote_copy(
                src_ref=fold_send.at[target, pl.ds(0, 2 * FOLD)],
                dst_ref=fold_recv.at[pz, pl.ds(0, 2 * FOLD)],
                send_sem=send_z_sem.at[c],
                recv_sem=recv_z_sem.at[c],
                device_id={"pz": target},
                device_id_type=mesh,
            )
        return pltpu.make_async_remote_copy(
            src_ref=send_z.at[c, target, pl.ds(0, X2)],
            dst_ref=recv_z.at[c, pz, pl.ds(0, X2)],
            send_sem=send_z_sem.at[c],
            recv_sem=recv_z_sem.at[c],
            device_id={"pz": target},
            device_id_type=mesh,
        )

    def send_planes(c, planes):
        for plane in planes:
            for core in (1, 0) if plane == 0 else (0, 1):
                target = 2 * plane + core

                @pl.when(pz != target)
                def _():
                    copy_z(c, target).start()

    def copy_y(c, target):
        return pltpu.make_async_remote_copy(
            src_ref=send_y.at[c, pl.ds(M2 * target, M2)],
            dst_ref=recv_y.at[c, pl.ds(M2 * py, M2)],
            send_sem=send_y_sem.at[c],
            recv_sem=recv_y_sem.at[c],
            device_id={"py": target},
            device_id_type=mesh,
        )

    def all_z(c):
        if c == 0:
            return pltpu.make_async_remote_copy(
                src_ref=fold_send.at[pl.ds(0, COLS - 1), pl.ds(0, 2 * FOLD)],
                dst_ref=fold_recv.at[pl.ds(0, COLS - 1), pl.ds(0, 2 * FOLD)],
                send_sem=send_z_sem.at[c],
                recv_sem=recv_z_sem.at[c],
                device_id={"pz": lax.rem(pz + 1, COLS)},
                device_id_type=mesh,
            )
        return pltpu.make_async_remote_copy(
            src_ref=send_z.at[c, pl.ds(0, COLS - 1), pl.ds(0, X2)],
            dst_ref=recv_z.at[c, pl.ds(0, COLS - 1), pl.ds(0, X2)],
            send_sem=send_z_sem.at[c],
            recv_sem=recv_z_sem.at[c],
            device_id={"pz": lax.rem(pz + 1, COLS)},
            device_id_type=mesh,
        )

    def all_y(c):
        return pltpu.make_async_remote_copy(
            src_ref=send_y.at[c, pl.ds(0, M2 * (ROWS - 1))],
            dst_ref=recv_y.at[c, pl.ds(0, M2 * (ROWS - 1))],
            send_sem=send_y_sem.at[c],
            recv_sem=recv_y_sem.at[c],
            device_id={"py": lax.rem(py + 1, ROWS)},
            device_id_type=mesh,
        )

    third_copy.wait()
    done_x = 0
    for c in range(CHUNKS):
        while done_x * FIELDS < STARTS[c + 1]:
            third_step(done_x)
            done_x += 1
        spread(c)
        if c == 0:
            fold()
            pl.semaphore_wait(barrier, COLS + ROWS - 2)
        if c < CHUNKS - 1:
            send_planes(c, PLANES)
        if c > 0:
            recv_z[c, pz, :X2] = send_z[c, pz, :X2]

    for planes in ((0, 2, 1), (3, 7, 4, 6, 5)):
        for c in range(CHUNKS - 1, CHUNKS):
            send_planes(c, planes)

    second_copy.wait()
    for c in range(CHUNKS):
        all_z(c).wait_recv()
        if c == 0:
            unfold()
        send_y[c] = dot(second_ref[...], recv_z[c].reshape(COLS * X2P, M))
        for target in TARGETS:

            @pl.when(py != target)
            def _():
                copy_y(c, target).start()


    first_copy.wait()
    coarse = [None] * FIELDS
    place = lax.broadcasted_iota(jnp.int32, (ROWS * M2, M), 0) // M2
    for c in range(CHUNKS):
        all_y(c).wait_recv()
        turned = jnp.where(place == py, send_y[c], recv_y[c]).T
        for x in range(X1):
            begin = max(x * FIELDS, STARTS[c])
            end = min((x + 1) * FIELDS, STARTS[c + 1])
            if begin >= end:
                continue
            rows = turned[M3 * (begin - STARTS[c]) : M3 * (end - STARTS[c])]
            own = lax.rem(lax.broadcasted_iota(jnp.int32, rows.shape, 1), M2)
            stacked = jnp.concatenate([jnp.where(own == m, rows, 0.0) for m in range(M2)], axis=0)
            done = dot(stacked, first_ref[x]).reshape(M2, end - begin, M3, M)
            for k in range(end - begin):
                f = begin + k - x * FIELDS
                if x == 0:
                    coarse_ref[f] = done[:, k]
                else:
                    coarse_ref[f] += done[:, k]

    for c in range(CHUNKS):
        all_z(c).wait_send()
        all_y(c).wait_send()


def finish(coarse_ref, filtered_ref, stress_ref):
    filtered_ref[...] = coarse_ref[:3]
    for p, (a, b) in enumerate(factor_pairs):
        stress_ref[p] = coarse_ref[3 + p] - coarse_ref[a] * coarse_ref[b]


def shards(velocity):
    third, second, first = (jnp.asarray(table, jnp.float32) for table in tables())
    vmem = pl.BlockSpec(memory_space=pltpu.VMEM)
    anywhere = pl.BlockSpec(memory_space=pl.ANY)
    f32 = jnp.float32
    coarse = pl.pallas_call(
        kernel,
        out_shape=jax.ShapeDtypeStruct((FIELDS, M2, M3, M), f32),
        in_specs=[anywhere] * 4,
        out_specs=vmem,
        scratch_shapes=[
            pltpu.VMEM((3, X1, X2, N), f32),
            pltpu.VMEM((N, M), f32),
            pltpu.VMEM((M, COLS * X2P), f32),
            pltpu.VMEM((X1, ROWS * M2, M), f32),
            pltpu.VMEM((X1 * FIELDS, X2P, M), f32),
            pltpu.VMEM((CHUNKS, COLS, X2P, M), f32),
            pltpu.VMEM((CHUNKS, COLS, X2P, M), f32),
            pltpu.VMEM((COLS, 16, M), f32),
            pltpu.VMEM((COLS, 16, M), f32),
            pltpu.VMEM((CHUNKS, ROWS * M2, M), f32),
            pltpu.VMEM((CHUNKS, ROWS * M2, M), f32),
            pltpu.SemaphoreType.DMA((X1,)),
            pltpu.SemaphoreType.DMA((3,)),
            pltpu.SemaphoreType.DMA((CHUNKS,)),
            pltpu.SemaphoreType.DMA((CHUNKS,)),
            pltpu.SemaphoreType.DMA((CHUNKS,)),
            pltpu.SemaphoreType.DMA((CHUNKS,)),
        ],
        compiler_params=pltpu.CompilerParams(collective_id=0, has_side_effects=True, vmem_limit_bytes=24 << 20),
    )(*(pltpu.with_memory_space_constraint(x, pltpu.HBM) for x in (velocity, third, second, first)))
    return pl.pallas_call(
        finish,
        out_shape=(
            jax.ShapeDtypeStruct((3, M2, M3, M), f32),
            jax.ShapeDtypeStruct((6, M2, M3, M), f32),
        ),
        in_specs=[vmem],
        out_specs=(vmem, vmem),
        compiler_params=pltpu.CompilerParams(vmem_limit_bytes=4 << 20),
    )(coarse)


def solution(mesh):
    placed = P(None, "py", "pz", None)
    return jax.shard_map(
        shards, mesh=mesh, in_specs=(placed,), out_specs=(placed, placed), check_vma=False
    )
```

```python
import math

import jax
import jax.numpy as jnp
import numpy as np
from jax import lax
from jax.experimental import pallas as pl
from jax.experimental.pallas import tpu as pltpu
from jax.sharding import PartitionSpec as P

N = 320
M = 128

factor_pairs = ((0, 0), (0, 1), (0, 2), (1, 1), (1, 2), (2, 2))
FIELDS = 3 + len(factor_pairs)
ROWS = 32
COLS = 16
X1 = N // ROWS
X2 = N // COLS
X2P = 24
M2 = M // ROWS
M3 = M // COLS
GROUP = 16
CHUNKS = -(-X1 * FIELDS // GROUP)
STARTS = [max(0, X1 * FIELDS - GROUP * (CHUNKS - c)) for c in range(CHUNKS + 1)]
HALF = M3 * STARTS[1] // 2
FOLD = 7
FOLDS = M // HALF
PLANES = (0, 1, 2, 3, 7, 4, 6, 5)


TARGETS = sorted(
    range(ROWS), key=lambda p: min(p // 4, 8 - p // 4) + min(p % 4, 4 - p % 4)
)


def filter_matrix():
    modes = np.arange(-(M // 2) + 1, M // 2)
    gain = np.exp(-(modes**2) * (2.0 * math.pi / M) ** 2 / 24.0)
    points = np.arange(M)[:, None, None] / M - np.arange(N)[None, :, None] / N
    return (np.cos(2.0 * math.pi * modes * points) * gain).sum(-1) / N


def tables():
    matrix = filter_matrix()
    second = np.zeros((M, COLS, X2P))
    second[:, :, :X2] = matrix.reshape(M, COLS, X2)
    first = np.repeat(matrix.T.reshape(ROWS, X1, M).transpose(1, 0, 2), M2, axis=1)
    return matrix.T.copy(), second.reshape(M, COLS * X2P), first


def dot(a, b):
    return lax.dot_general(
        a,
        b,
        (((1,), (0,)), ((), ())),
        precision=lax.Precision.HIGHEST,
        preferred_element_type=jnp.float32,
    )


def kernel(
    v_hbm,
    third_hbm,
    second_hbm,
    first_hbm,
    coarse_ref,
    v_ref,
    third_ref,
    second_ref,
    first_ref,
    wide_ref,
    mixed,
    send_z,
    recv_z,
    fold_send,
    fold_recv,
    send_y,
    recv_y,
    v_sem,
    table_sem,
    send_z_sem,
    recv_z_sem,
    send_y_sem,
    recv_y_sem,
):
    py = lax.axis_index("py")
    pz = lax.axis_index("pz")
    mesh = pl.DeviceIdType.MESH

    v_copies = [
        pltpu.make_async_copy(v_hbm.at[:, x], v_ref.at[:, x], v_sem.at[x]) for x in range(X1)
    ]
    third_copy = pltpu.make_async_copy(third_hbm, third_ref, table_sem.at[0])
    second_copy = pltpu.make_async_copy(second_hbm, second_ref, table_sem.at[1])
    first_copy = pltpu.make_async_copy(first_hbm, first_ref, table_sem.at[2])
    third_copy.start()
    for copy in v_copies:
        copy.start()
    second_copy.start()
    first_copy.start()

    barrier = pltpu.get_barrier_semaphore()
    for step in range(1, COLS):
        pl.semaphore_signal(
            barrier, inc=1, device_id={"pz": lax.rem(pz + step, COLS)}, device_id_type=mesh
        )
    for step in range(1, ROWS):
        pl.semaphore_signal(
            barrier, inc=1, device_id={"py": lax.rem(py + step, ROWS)}, device_id_type=mesh
        )

    recv_z[:, :, X2:, :] = jnp.zeros((CHUNKS, COLS, X2P - X2, M), jnp.float32)
    lanes = lax.broadcasted_iota(jnp.int32, (8, M), 1)

    def third_step(x):
        v_copies[x].wait()
        pad = jnp.zeros((X2P - X2, N), jnp.float32)
        parts = [jnp.concatenate([v_ref[c, x], pad], axis=0) for c in range(3)]
        parts = parts + [parts[a] * parts[b] for a, b in factor_pairs]
        done = dot(jnp.concatenate(parts, axis=0), third_ref[...])
        mixed[x * FIELDS : (x + 1) * FIELDS] = done.reshape(FIELDS, X2P, M)

    def spread(c):
        for r in range(X2P // 8):
            pairs = range(STARTS[c], STARTS[c + 1])
            tiles = [mixed[k, 8 * r : 8 * r + 8, :] for k in pairs]
            tiles = tiles + [jnp.zeros((8, M), jnp.float32)] * (GROUP - len(pairs))
            for b in (8, 4, 2, 1):
                low = (lanes // (M3 * b)) % 2 == 0
                for k in range(GROUP):
                    if k & b == 0:
                        x, y = tiles[k], tiles[k + b]
                        tiles[k] = jnp.where(low, x, pltpu.roll(y, M3 * b, 1))
                        tiles[k + b] = jnp.where(low, pltpu.roll(x, M - M3 * b, 1), y)
            for t in range(COLS):
                send_z[c, t, 8 * r : 8 * r + 8, :] = tiles[t]

    def fold():
        for t in range(COLS):
            for half in range(2):
                row = jnp.zeros((8, M), jnp.float32)
                for g in range(FOLDS):
                    part = send_z[0, t, FOLD * g : FOLD * g + 8, :]
                    part = pltpu.roll(part, (HALF * (g - half)) % M, 1) if g != half else part
                    row = jnp.where(lanes // HALF == g, part, row)
                fold_send[t, FOLD * half : FOLD * half + 8, :] = row

    def unfold():
        for t in range(COLS):
            for g in range(FOLDS):
                row = jnp.zeros((8, M), jnp.float32)
                for half in range(2):
                    part = fold_recv[t, FOLD * half : FOLD * half + 8, :]
                    part = pltpu.roll(part, (HALF * (half - g)) % M, 1) if g != half else part
                    row = jnp.where(lanes // HALF == half, part, row)
                kept = min(8, X2 - FOLD * g)
                recv_z[0, t, FOLD * g : FOLD * g + kept, :] = row[:kept]
        recv_z[0, pz, :X2] = send_z[0, pz, :X2]

    def copy_z(c, target):
        if c == 0:
            return pltpu.make_async_remote_copy(
                src_ref=fold_send.at[target, pl.ds(0, 2 * FOLD)],
                dst_ref=fold_recv.at[pz, pl.ds(0, 2 * FOLD)],
                send_sem=send_z_sem.at[c],
                recv_sem=recv_z_sem.at[c],
                device_id={"pz": target},
                device_id_type=mesh,
            )
        return pltpu.make_async_remote_copy(
            src_ref=send_z.at[c, target, pl.ds(0, X2)],
            dst_ref=recv_z.at[c, pz, pl.ds(0, X2)],
            send_sem=send_z_sem.at[c],
            recv_sem=recv_z_sem.at[c],
            device_id={"pz": target},
            device_id_type=mesh,
        )

    def send_planes(c, planes):
        for plane in planes:
            for core in (1, 0) if plane == 0 else (0, 1):
                target = 2 * plane + core

                @pl.when(pz != target)
                def _():
                    copy_z(c, target).start()

    def copy_y(c, target):
        return pltpu.make_async_remote_copy(
            src_ref=send_y.at[c, pl.ds(M2 * target, M2)],
            dst_ref=recv_y.at[c, pl.ds(M2 * py, M2)],
            send_sem=send_y_sem.at[c],
            recv_sem=recv_y_sem.at[c],
            device_id={"py": target},
            device_id_type=mesh,
        )

    def all_z(c):
        if c == 0:
            return pltpu.make_async_remote_copy(
                src_ref=fold_send.at[pl.ds(0, COLS - 1), pl.ds(0, 2 * FOLD)],
                dst_ref=fold_recv.at[pl.ds(0, COLS - 1), pl.ds(0, 2 * FOLD)],
                send_sem=send_z_sem.at[c],
                recv_sem=recv_z_sem.at[c],
                device_id={"pz": lax.rem(pz + 1, COLS)},
                device_id_type=mesh,
            )
        return pltpu.make_async_remote_copy(
            src_ref=send_z.at[c, pl.ds(0, COLS - 1), pl.ds(0, X2)],
            dst_ref=recv_z.at[c, pl.ds(0, COLS - 1), pl.ds(0, X2)],
            send_sem=send_z_sem.at[c],
            recv_sem=recv_z_sem.at[c],
            device_id={"pz": lax.rem(pz + 1, COLS)},
            device_id_type=mesh,
        )

    def all_y(c):
        return pltpu.make_async_remote_copy(
            src_ref=send_y.at[c, pl.ds(0, M2 * (ROWS - 1))],
            dst_ref=recv_y.at[c, pl.ds(0, M2 * (ROWS - 1))],
            send_sem=send_y_sem.at[c],
            recv_sem=recv_y_sem.at[c],
            device_id={"py": lax.rem(py + 1, ROWS)},
            device_id_type=mesh,
        )

    third_copy.wait()
    done_x = 0
    for c in range(CHUNKS):
        while done_x * FIELDS < STARTS[c + 1]:
            third_step(done_x)
            done_x += 1
        spread(c)
        if c == 0:
            fold()
            pl.semaphore_wait(barrier, COLS + ROWS - 2)
        if c < CHUNKS - 1:
            send_planes(c, PLANES)
        if c > 0:
            recv_z[c, pz, :X2] = send_z[c, pz, :X2]

    for planes in ((0, 1, 2), (3, 7, 4, 6, 5)):
        for c in range(CHUNKS - 1, CHUNKS):
            send_planes(c, planes)

    first_copy.wait()
    own = lax.rem(lax.broadcasted_iota(jnp.int32, (ROWS * M2, M), 0), M2)
    for x in range(X1):
        for m in range(M2):
            wide_ref[x, :, M * m : M * (m + 1)] = jnp.where(own == m, first_ref[x], 0.0)
    second_copy.wait()
    for c in range(CHUNKS):
        all_z(c).wait_recv()
        if c == 0:
            unfold()
        send_y[c] = dot(second_ref[...], recv_z[c].reshape(COLS * X2P, M))
        for target in TARGETS:

            @pl.when(py != target)
            def _():
                copy_y(c, target).start()


    coarse = [None] * FIELDS
    place = lax.broadcasted_iota(jnp.int32, (ROWS * M2, M), 0) // M2
    for c in range(CHUNKS):
        all_y(c).wait_recv()
        turned = jnp.where(place == py, send_y[c], recv_y[c]).T
        for x in range(X1):
            begin = max(x * FIELDS, STARTS[c])
            end = min((x + 1) * FIELDS, STARTS[c + 1])
            if begin >= end:
                continue
            rows = turned[M3 * (begin - STARTS[c]) : M3 * (end - STARTS[c])]
            done = dot(rows, wide_ref[x])
            for k in range(end - begin):
                f = begin + k - x * FIELDS
                for m in range(M2):
                    tile = done[M3 * k : M3 * (k + 1), M * m : M * (m + 1)]
                    if x == 0:
                        coarse_ref[f, m] = tile
                    else:
                        coarse_ref[f, m] += tile

    for c in range(CHUNKS):
        all_z(c).wait_send()
        all_y(c).wait_send()


def finish(coarse_ref, filtered_ref, stress_ref):
    filtered_ref[...] = coarse_ref[:3]
    for p, (a, b) in enumerate(factor_pairs):
        stress_ref[p] = coarse_ref[3 + p] - coarse_ref[a] * coarse_ref[b]


def shards(velocity):
    third, second, first = (jnp.asarray(table, jnp.float32) for table in tables())
    vmem = pl.BlockSpec(memory_space=pltpu.VMEM)
    anywhere = pl.BlockSpec(memory_space=pl.ANY)
    f32 = jnp.float32
    coarse = pl.pallas_call(
        kernel,
        out_shape=jax.ShapeDtypeStruct((FIELDS, M2, M3, M), f32),
        in_specs=[anywhere] * 4,
        out_specs=vmem,
        scratch_shapes=[
            pltpu.VMEM((3, X1, X2, N), f32),
            pltpu.VMEM((N, M), f32),
            pltpu.VMEM((M, COLS * X2P), f32),
            pltpu.VMEM((X1, ROWS * M2, M), f32),
            pltpu.VMEM((X1, ROWS * M2, M2 * M), f32),
            pltpu.VMEM((X1 * FIELDS, X2P, M), f32),
            pltpu.VMEM((CHUNKS, COLS, X2P, M), f32),
            pltpu.VMEM((CHUNKS, COLS, X2P, M), f32),
            pltpu.VMEM((COLS, 16, M), f32),
            pltpu.VMEM((COLS, 16, M), f32),
            pltpu.VMEM((CHUNKS, ROWS * M2, M), f32),
            pltpu.VMEM((CHUNKS, ROWS * M2, M), f32),
            pltpu.SemaphoreType.DMA((X1,)),
            pltpu.SemaphoreType.DMA((3,)),
            pltpu.SemaphoreType.DMA((CHUNKS,)),
            pltpu.SemaphoreType.DMA((CHUNKS,)),
            pltpu.SemaphoreType.DMA((CHUNKS,)),
            pltpu.SemaphoreType.DMA((CHUNKS,)),
        ],
        compiler_params=pltpu.CompilerParams(collective_id=0, has_side_effects=True, vmem_limit_bytes=24 << 20),
    )(*(pltpu.with_memory_space_constraint(x, pltpu.HBM) for x in (velocity, third, second, first)))
    return pl.pallas_call(
        finish,
        out_shape=(
            jax.ShapeDtypeStruct((3, M2, M3, M), f32),
            jax.ShapeDtypeStruct((6, M2, M3, M), f32),
        ),
        in_specs=[vmem],
        out_specs=(vmem, vmem),
        compiler_params=pltpu.CompilerParams(vmem_limit_bytes=4 << 20),
    )(coarse)


def solution(mesh):
    placed = P(None, "py", "pz", None)
    return jax.shard_map(
        shards, mesh=mesh, in_specs=(placed,), out_specs=(placed, placed), check_vma=False
    )
```

```python
import math

import jax
import jax.numpy as jnp
import numpy as np
from jax import lax
from jax.experimental import pallas as pl
from jax.experimental.pallas import tpu as pltpu
from jax.sharding import PartitionSpec as P

N = 320
M = 128

factor_pairs = ((0, 0), (0, 1), (0, 2), (1, 1), (1, 2), (2, 2))
FIELDS = 3 + len(factor_pairs)
ROWS = 32
COLS = 16
X1 = N // ROWS
X2 = N // COLS
X2P = 24
M2 = M // ROWS
M3 = M // COLS
GROUP = 16
CHUNKS = -(-X1 * FIELDS // GROUP)
STARTS = [max(0, X1 * FIELDS - GROUP * (CHUNKS - c)) for c in range(CHUNKS + 1)]
HALF = M3 * STARTS[1] // 2
FOLD = 7
FOLDS = M // HALF
PLANES = (0, 1, 2, 3, 7, 4, 6, 5)


TARGETS = sorted(
    range(ROWS), key=lambda p: min(p // 4, 8 - p // 4) + min(p % 4, 4 - p % 4)
)


def filter_matrix():
    modes = np.arange(-(M // 2) + 1, M // 2)
    gain = np.exp(-(modes**2) * (2.0 * math.pi / M) ** 2 / 24.0)
    points = np.arange(M)[:, None, None] / M - np.arange(N)[None, :, None] / N
    return (np.cos(2.0 * math.pi * modes * points) * gain).sum(-1) / N


def tables():
    matrix = filter_matrix()
    second = np.zeros((M, COLS, X2P))
    second[:, :, :X2] = matrix.reshape(M, COLS, X2)
    first = np.repeat(matrix.T.reshape(ROWS, X1, M).transpose(1, 0, 2), M2, axis=1)
    return matrix.T.copy(), second.reshape(M, COLS * X2P), first


def dot(a, b):
    return lax.dot_general(
        a,
        b,
        (((1,), (0,)), ((), ())),
        precision=lax.Precision.HIGHEST,
        preferred_element_type=jnp.float32,
    )


def kernel(
    v_hbm,
    third_hbm,
    second_hbm,
    first_hbm,
    coarse_ref,
    v_ref,
    third_ref,
    second_ref,
    first_ref,
    wide_ref,
    mixed,
    send_z,
    recv_z,
    fold_send,
    fold_recv,
    send_y,
    recv_y,
    v_sem,
    table_sem,
    send_z_sem,
    recv_z_sem,
    send_y_sem,
    recv_y_sem,
):
    py = lax.axis_index("py")
    pz = lax.axis_index("pz")
    mesh = pl.DeviceIdType.MESH

    v_copies = [
        pltpu.make_async_copy(v_hbm.at[:, x], v_ref.at[:, x], v_sem.at[x]) for x in range(X1)
    ]
    third_copy = pltpu.make_async_copy(third_hbm, third_ref, table_sem.at[0])
    second_copy = pltpu.make_async_copy(second_hbm, second_ref, table_sem.at[1])
    first_copy = pltpu.make_async_copy(first_hbm, first_ref, table_sem.at[2])
    barrier = pltpu.get_barrier_semaphore()
    for step in range(1, COLS):
        pl.semaphore_signal(
            barrier, inc=1, device_id={"pz": lax.rem(pz + step, COLS)}, device_id_type=mesh
        )
    for step in range(1, ROWS):
        pl.semaphore_signal(
            barrier, inc=1, device_id={"py": lax.rem(py + step, ROWS)}, device_id_type=mesh
        )

    third_copy.start()
    for copy in v_copies:
        copy.start()
    second_copy.start()
    first_copy.start()

    recv_z[:, :, X2:, :] = jnp.zeros((CHUNKS, COLS, X2P - X2, M), jnp.float32)
    lanes = lax.broadcasted_iota(jnp.int32, (8, M), 1)

    def third_step(x):
        v_copies[x].wait()
        pad = jnp.zeros((X2P - X2, N), jnp.float32)
        parts = [jnp.concatenate([v_ref[c, x], pad], axis=0) for c in range(3)]
        parts = parts + [parts[a] * parts[b] for a, b in factor_pairs]
        done = dot(jnp.concatenate(parts, axis=0), third_ref[...])
        mixed[x * FIELDS : (x + 1) * FIELDS] = done.reshape(FIELDS, X2P, M)

    def spread(c):
        for r in range(X2P // 8):
            pairs = range(STARTS[c], STARTS[c + 1])
            tiles = [mixed[k, 8 * r : 8 * r + 8, :] for k in pairs]
            tiles = tiles + [jnp.zeros((8, M), jnp.float32)] * (GROUP - len(pairs))
            for b in (8, 4, 2, 1):
                low = (lanes // (M3 * b)) % 2 == 0
                for k in range(GROUP):
                    if k & b == 0:
                        x, y = tiles[k], tiles[k + b]
                        tiles[k] = jnp.where(low, x, pltpu.roll(y, M3 * b, 1))
                        tiles[k + b] = jnp.where(low, pltpu.roll(x, M - M3 * b, 1), y)
            for t in range(COLS):
                send_z[c, t, 8 * r : 8 * r + 8, :] = tiles[t]

    def fold():
        for t in range(COLS):
            for half in range(2):
                row = jnp.zeros((8, M), jnp.float32)
                for g in range(FOLDS):
                    part = send_z[0, t, FOLD * g : FOLD * g + 8, :]
                    part = pltpu.roll(part, (HALF * (g - half)) % M, 1) if g != half else part
                    row = jnp.where(lanes // HALF == g, part, row)
                fold_send[t, FOLD * half : FOLD * half + 8, :] = row

    def unfold():
        for t in range(COLS):
            for g in range(FOLDS):
                row = jnp.zeros((8, M), jnp.float32)
                for half in range(2):
                    part = fold_recv[t, FOLD * half : FOLD * half + 8, :]
                    part = pltpu.roll(part, (HALF * (half - g)) % M, 1) if g != half else part
                    row = jnp.where(lanes // HALF == half, part, row)
                kept = min(8, X2 - FOLD * g)
                recv_z[0, t, FOLD * g : FOLD * g + kept, :] = row[:kept]
        recv_z[0, pz, :X2] = send_z[0, pz, :X2]

    def copy_z(c, target):
        if c == 0:
            return pltpu.make_async_remote_copy(
                src_ref=fold_send.at[target, pl.ds(0, 2 * FOLD)],
                dst_ref=fold_recv.at[pz, pl.ds(0, 2 * FOLD)],
                send_sem=send_z_sem.at[c],
                recv_sem=recv_z_sem.at[c],
                device_id={"pz": target},
                device_id_type=mesh,
            )
        return pltpu.make_async_remote_copy(
            src_ref=send_z.at[c, target, pl.ds(0, X2)],
            dst_ref=recv_z.at[c, pz, pl.ds(0, X2)],
            send_sem=send_z_sem.at[c],
            recv_sem=recv_z_sem.at[c],
            device_id={"pz": target},
            device_id_type=mesh,
        )

    def send_planes(c, planes):
        for plane in planes:
            for core in (1, 0) if plane == 0 else (0, 1):
                target = 2 * plane + core

                @pl.when(pz != target)
                def _():
                    copy_z(c, target).start()

    def copy_y(c, target):
        return pltpu.make_async_remote_copy(
            src_ref=send_y.at[c, pl.ds(M2 * target, M2)],
            dst_ref=recv_y.at[c, pl.ds(M2 * py, M2)],
            send_sem=send_y_sem.at[c],
            recv_sem=recv_y_sem.at[c],
            device_id={"py": target},
            device_id_type=mesh,
        )

    def all_z(c):
        if c == 0:
            return pltpu.make_async_remote_copy(
                src_ref=fold_send.at[pl.ds(0, COLS - 1), pl.ds(0, 2 * FOLD)],
                dst_ref=fold_recv.at[pl.ds(0, COLS - 1), pl.ds(0, 2 * FOLD)],
                send_sem=send_z_sem.at[c],
                recv_sem=recv_z_sem.at[c],
                device_id={"pz": lax.rem(pz + 1, COLS)},
                device_id_type=mesh,
            )
        return pltpu.make_async_remote_copy(
            src_ref=send_z.at[c, pl.ds(0, COLS - 1), pl.ds(0, X2)],
            dst_ref=recv_z.at[c, pl.ds(0, COLS - 1), pl.ds(0, X2)],
            send_sem=send_z_sem.at[c],
            recv_sem=recv_z_sem.at[c],
            device_id={"pz": lax.rem(pz + 1, COLS)},
            device_id_type=mesh,
        )

    def all_y(c):
        return pltpu.make_async_remote_copy(
            src_ref=send_y.at[c, pl.ds(0, M2 * (ROWS - 1))],
            dst_ref=recv_y.at[c, pl.ds(0, M2 * (ROWS - 1))],
            send_sem=send_y_sem.at[c],
            recv_sem=recv_y_sem.at[c],
            device_id={"py": lax.rem(py + 1, ROWS)},
            device_id_type=mesh,
        )

    third_copy.wait()
    done_x = 0
    for c in range(CHUNKS):
        while done_x * FIELDS < STARTS[c + 1]:
            third_step(done_x)
            done_x += 1
        spread(c)
        if c == 0:
            fold()
            pl.semaphore_wait(barrier, COLS + ROWS - 2)
        if c < CHUNKS - 1:
            send_planes(c, PLANES)
        if c > 0:
            recv_z[c, pz, :X2] = send_z[c, pz, :X2]

    for planes in ((0, 1, 2), (3, 7, 4, 6, 5)):
        for c in range(CHUNKS - 1, CHUNKS):
            send_planes(c, planes)

    first_copy.wait()
    own = lax.rem(lax.broadcasted_iota(jnp.int32, (ROWS * M2, M), 0), M2)
    for x in range(X1):
        for m in range(M2):
            wide_ref[x, :, M * m : M * (m + 1)] = jnp.where(own == m, first_ref[x], 0.0)
    second_copy.wait()
    for c in range(CHUNKS):
        all_z(c).wait_recv()
        if c == 0:
            unfold()
        send_y[c] = dot(second_ref[...], recv_z[c].reshape(COLS * X2P, M))
        for target in TARGETS:

            @pl.when(py != target)
            def _():
                copy_y(c, target).start()


    coarse = [None] * FIELDS
    place = lax.broadcasted_iota(jnp.int32, (ROWS * M2, M), 0) // M2
    for c in range(CHUNKS):
        all_y(c).wait_recv()
        turned = jnp.where(place == py, send_y[c], recv_y[c]).T
        for x in range(X1):
            begin = max(x * FIELDS, STARTS[c])
            end = min((x + 1) * FIELDS, STARTS[c + 1])
            if begin >= end:
                continue
            rows = turned[M3 * (begin - STARTS[c]) : M3 * (end - STARTS[c])]
            done = dot(rows, wide_ref[x])
            for k in range(end - begin):
                f = begin + k - x * FIELDS
                for m in range(M2):
                    tile = done[M3 * k : M3 * (k + 1), M * m : M * (m + 1)]
                    if x == 0:
                        coarse_ref[f, m] = tile
                    else:
                        coarse_ref[f, m] += tile

    for c in range(CHUNKS):
        all_z(c).wait_send()
        all_y(c).wait_send()


def finish(coarse_ref, filtered_ref, stress_ref):
    filtered_ref[...] = coarse_ref[:3]
    for p, (a, b) in enumerate(factor_pairs):
        stress_ref[p] = coarse_ref[3 + p] - coarse_ref[a] * coarse_ref[b]


def shards(velocity):
    third, second, first = (jnp.asarray(table, jnp.float32) for table in tables())
    vmem = pl.BlockSpec(memory_space=pltpu.VMEM)
    anywhere = pl.BlockSpec(memory_space=pl.ANY)
    f32 = jnp.float32
    coarse = pl.pallas_call(
        kernel,
        out_shape=jax.ShapeDtypeStruct((FIELDS, M2, M3, M), f32),
        in_specs=[anywhere] * 4,
        out_specs=vmem,
        scratch_shapes=[
            pltpu.VMEM((3, X1, X2, N), f32),
            pltpu.VMEM((N, M), f32),
            pltpu.VMEM((M, COLS * X2P), f32),
            pltpu.VMEM((X1, ROWS * M2, M), f32),
            pltpu.VMEM((X1, ROWS * M2, M2 * M), f32),
            pltpu.VMEM((X1 * FIELDS, X2P, M), f32),
            pltpu.VMEM((CHUNKS, COLS, X2P, M), f32),
            pltpu.VMEM((CHUNKS, COLS, X2P, M), f32),
            pltpu.VMEM((COLS, 16, M), f32),
            pltpu.VMEM((COLS, 16, M), f32),
            pltpu.VMEM((CHUNKS, ROWS * M2, M), f32),
            pltpu.VMEM((CHUNKS, ROWS * M2, M), f32),
            pltpu.SemaphoreType.DMA((X1,)),
            pltpu.SemaphoreType.DMA((3,)),
            pltpu.SemaphoreType.DMA((CHUNKS,)),
            pltpu.SemaphoreType.DMA((CHUNKS,)),
            pltpu.SemaphoreType.DMA((CHUNKS,)),
            pltpu.SemaphoreType.DMA((CHUNKS,)),
        ],
        compiler_params=pltpu.CompilerParams(collective_id=0, has_side_effects=True, vmem_limit_bytes=24 << 20),
    )(*(pltpu.with_memory_space_constraint(x, pltpu.HBM) for x in (velocity, third, second, first)))
    return pl.pallas_call(
        finish,
        out_shape=(
            jax.ShapeDtypeStruct((3, M2, M3, M), f32),
            jax.ShapeDtypeStruct((6, M2, M3, M), f32),
        ),
        in_specs=[vmem],
        out_specs=(vmem, vmem),
        compiler_params=pltpu.CompilerParams(vmem_limit_bytes=4 << 20),
    )(coarse)


def solution(mesh):
    placed = P(None, "py", "pz", None)
    return jax.shard_map(
        shards, mesh=mesh, in_specs=(placed,), out_specs=(placed, placed), check_vma=False
    )
```
